32 devices in a mesh: tm: 16 (over z, y, x), chan: 2 (over core).
Axes of the slice: x: 2, y: 2, z: 4, core: 2. Of those that a mesh axis runs over, the one named last changes fastest.
Arguments:
- spectrum: float32 [32, 131072], P('tm', 'chan'), may hold values from -6 to 6
- offsets: int32 [64], replicated, may hold values from 0 to 16, as said below
Outputs:
- peak: float32 [131072], P('chan')
The draws below stay inside these ranges and needn't reach their ends.
Inputs may be any that keep to these rules, and one draw needn't show every extreme that they name: `offsets`: entries 0 and 1 are 0; entry 2L + d (drift d of the section that joins blocks of L) lies in 0 to L, and is exactly L for d = 2L - 1.
All inputs are finite; a program needn't handle non-finite values.
Results may differ from the reference program's by a relative error of at most 0.00002.
Values sent between devices are 32-bit elements; how exact they have to be, the bound alone decides.
A program may use at most 64 MiB of HBM per device.

```python
import jax
import jax.numpy as jnp
from jax import lax

TOTAL = 32
CHANNELS = 131072


def draw_offsets(key, part):
    count = 2 * TOTAL
    places = jnp.arange(count, dtype=jnp.int32)
    section = jnp.where(places >= 2, 1, 0).astype(jnp.int32)
    for power in range(1, 24):
        section = jnp.where(places >= 2 ** (power + 1), 2 ** power, section).astype(jnp.int32)
    drift = places - 2 * section
    jitter = jax.random.randint(jax.random.fold_in(key, 7), (count,), -1, 2).astype(jnp.int32)
    value = jnp.clip((drift + 1) // 2 + jitter, 0, section)
    value = jnp.where(drift == 2 * section - 1, section, value)
    value = jnp.where(places < 2, 0, value)
    return value.astype(jnp.int32)


def shard_levels(rng, shape, split, low, high):
    def one(axis_at, shards_of):
        draws = jax.random.uniform(jax.random.fold_in(jax.random.fold_in(rng, 6), axis_at), (shards_of,), jnp.float32, low / len(split), high / len(split))
        return jnp.repeat(jnp.exp(draws), shape[axis_at] // shards_of).reshape((-1,) + (1,) * (len(shape) - axis_at - 1))

    loudness = one(*split[0])
    for cut in split[1:]:
        loudness = loudness * one(*cut)
    return loudness


def noise(stream_key, extent, deviation, limit, cuts=(), kind=jnp.bfloat16):
    values = jax.random.normal(stream_key, extent, jnp.float32) * deviation
    if len(cuts) > 0:
        values = shard_levels(stream_key, extent, cuts, -0.22, 0.18) * values
    return jnp.clip(values, min=-limit, max=limit).astype(kind)


def setup_inputs(seed: int = 0) -> dict:
    splits = jax.random.split(jax.random.key(seed), 3)
    spectrum = noise(splits[0], (TOTAL, CHANNELS), 1.0, 6.0, ((0, 16), (1, 2)), jnp.float32)
    offsets = draw_offsets(jax.random.fold_in(splits[2], 71), 0)
    return {"spectrum": spectrum, "offsets": offsets}


def take_window(single, amount, span_cols):
    return lax.dynamic_slice_in_dim(single, amount, span_cols)


def combine(lower_rows, upper_ext, shifts, span_cols):
    upper_two = jnp.repeat(upper_ext, 2, axis=0)
    moved = jax.vmap(take_window, in_axes=(0, 0, None))(upper_two, shifts, span_cols)
    return jnp.repeat(lower_rows[:, :span_cols], 2, axis=0) + moved


def reference(spectrum, offsets):
    total = spectrum.shape[0]
    channels = spectrum.shape[1]
    sums = spectrum
    length = 1
    while length < total:
        blocks = total // (2 * length)
        paired = sums.reshape(blocks, 2, length, channels)
        lower_rows = paired[:, 0].reshape(blocks * length, channels)
        upper_rows = paired[:, 1].reshape(blocks * length, channels)
        upper_ext = jnp.pad(upper_rows, ((0, 0), (0, length)))
        shifts = jnp.tile(offsets[2 * length:4 * length], blocks).astype(jnp.int32)
        sums = combine(lower_rows, upper_ext, shifts, channels)
        length = length * 2
    return jnp.max(sums, axis=0)
```

```python
import functools

import jax
import jax.numpy as jnp
from jax import lax
from jax.experimental import pallas as pl
from jax.experimental.pallas import tpu as pltpu
from jax.sharding import PartitionSpec as P

LANES = 128
MESH = pl.DeviceIdType.MESH


def round_up(value, to):
    return (value + to - 1) // to * to


def flip(place, bits):
    out, bit = place, 1
    while bit <= bits:
        if bits & bit:
            out = out + bit * (1 - 2 * lax.rem(lax.div(place, bit), 2))
        bit *= 2
    return out


def kernel(count, chans, rows, tiles, halo, offs_ref, x_ref, out_ref, recv, *rest):
    levels = rest[:-5]
    send_sem, recv_sem, edge_sem, send_sem2, recv_sem2 = rest[-5:]
    me = lax.axis_index("tm")
    col = lax.axis_index("chan")
    total = count * rows
    body = tiles
    full = tiles + halo
    at_end = me == count - 1
    no_next = me * chans + col == count * chans - 1

    barrier = pltpu.get_barrier_semaphore()
    for j in range(1, count):
        pl.semaphore_signal(barrier, inc=1, device_id=(flip(me, j), col), device_id_type=MESH)
    if chans > 1:
        @pl.when(jnp.logical_and(at_end, col < chans - 1))
        def _():
            for t in range(count):
                pl.semaphore_signal(barrier, inc=1, device_id=(t, jnp.minimum(col + 1, chans - 1)), device_id_type=MESH)
    pl.semaphore_wait(barrier, count - 1 + jnp.where(col > 0, 1, 0))

    def to_peer(j, size):
        k = flip(me, j)
        return pltpu.make_async_remote_copy(
            src_ref=x_ref.at[pl.ds(k * body, size)],
            dst_ref=recv.at[me, pl.ds(0, size)],
            send_sem=send_sem.at[j],
            recv_sem=recv_sem.at[me],
            device_id=(k, col),
            device_id_type=MESH,
        )

    def both(j, act):
        @pl.when(flip(me, j) == count - 1)
        def _():
            act(to_peer(j, body))

        @pl.when(flip(me, j) != count - 1)
        def _():
            act(to_peer(j, full))

    def edge():
        return pltpu.make_async_remote_copy(
            src_ref=x_ref.at[pl.ds(0, halo)],
            dst_ref=recv.at[me, pl.ds(body, halo)],
            send_sem=edge_sem.at[0],
            recv_sem=recv_sem.at[me],
            device_id=(count - 1, jnp.maximum(col - 1, 0)),
            device_id_type=MESH,
        )

    def own(size):
        return pltpu.make_async_copy(
            x_ref.at[pl.ds(me * body, size)], recv.at[me, pl.ds(0, size)], recv_sem.at[me]
        )

    for j in reversed(range(1, count)):
        both(j, lambda copy: copy.start())
    if chans > 1:
        @pl.when(col > 0)
        def _():
            edge().start()

    @pl.when(at_end)
    def _():
        own(body).start()

    @pl.when(me != count - 1)
    def _():
        own(full).start()

    @pl.when(no_next)
    def _():
        for t in range(count):
            recv[t, pl.ds(body, halo)] = jnp.zeros((halo, rows, LANES), jnp.float32)

    def arrived(t):
        def wait(size):
            part = recv.at[t, pl.ds(0, size)]
            pltpu.make_async_copy(part, part, recv_sem.at[t]).wait()

        @pl.when(no_next)
        def _():
            wait(body)

        @pl.when(me * chans + col != count * chans - 1)
        def _():
            wait(full)

    def node(length, block, slot=0, inner=0):
        at = length.bit_length() - 1
        wide = tiles + (total - 2 * length + LANES - 1) // LANES
        lane = lax.broadcasted_iota(jnp.int32, (wide, LANES), 1)

        def load(which, d, start):
            if length == 1:
                return recv[slot, pl.ds(start, wide), 2 * inner + which]
            return levels[at - 1][2 * block + which, d, pl.ds(start, wide)]

        peak = None
        for half in range(length):
            low = load(0, half, 0)
            here = load(1, half, 0)
            ahead = load(1, half, 1)
            for d in (2 * half, 2 * half + 1):
                by = offs_ref[2 * length + d]
                mixed = jnp.where(lane >= by, here, ahead)
                value = low + pltpu.roll(mixed, lax.rem(LANES - by, LANES), 1)
                if 2 * length < total:
                    levels[at][block, d, pl.ds(0, wide)] = value
                else:
                    peak = value if peak is None else jnp.maximum(peak, value)
        return peak

    peak = None
    for j in range(count):
        slot = flip(me, j)
        arrived(slot)
        length = 1
        while length < rows:
            for inner in range(rows // (2 * length)):
                peak = node(length, slot * (rows // (2 * length)) + inner, slot, inner)
            length *= 2
        step = 1
        while step < count and (j + 1) % (2 * step) == 0:
            peak = node(step * rows, flip(lax.div(me, 2 * step), j // (2 * step)))
            step *= 2

    mine = pl.ds(me * tiles, tiles)
    out_ref[mine] = peak
    for j in range(1, count):
        both(j, lambda copy: copy.wait_send())
    if chans > 1:
        @pl.when(col > 0)
        def _():
            edge().wait_send()

    def result(j, t):
        part = out_ref.at[pl.ds(t * tiles, tiles)]
        return pltpu.make_async_remote_copy(
            src_ref=part,
            dst_ref=part,
            send_sem=send_sem2.at[j],
            recv_sem=recv_sem2.at[t],
            device_id=(flip(me, j), col),
            device_id_type=MESH,
        )

    for j in reversed(range(1, count)):
        result(j, me).start()
    for j in range(1, count):
        result(j, flip(me, j)).wait_recv()
    for j in range(1, count):
        result(j, me).wait_send()


def local(count, chans, spectrum, offsets):
    rows, span = spectrum.shape
    total = count * rows
    tiles = span // LANES // count
    halo = (total - 1 + LANES - 1) // LANES
    x = spectrum.reshape(rows, span // LANES, LANES).transpose(1, 0, 2)
    deep = round_up(tiles + halo, 8) + 8
    scratch = [pltpu.VMEM((count, deep, rows, LANES), jnp.float32)]
    length = 2
    while length < total:
        scratch.append(pltpu.VMEM((total // length, length, deep, LANES), jnp.float32))
        length *= 2
    dma = pltpu.SemaphoreType.DMA
    scratch += [dma((count,)), dma((count,)), dma((1,)), dma((count,)), dma((count,))]
    peak = pl.pallas_call(
        functools.partial(kernel, count, chans, rows, tiles, halo),
        out_shape=jax.ShapeDtypeStruct((count * tiles, LANES), jnp.float32),
        in_specs=[pl.BlockSpec(memory_space=pltpu.SMEM), pl.BlockSpec(memory_space=pl.ANY)],
        out_specs=pl.BlockSpec(memory_space=pltpu.VMEM),
        scratch_shapes=scratch,
        compiler_params=pltpu.CompilerParams(collective_id=0, has_side_effects=True),
    )(offsets, x)
    return peak.reshape(span)


def solution(mesh):
    body = functools.partial(local, mesh.shape["tm"], mesh.shape["chan"])
    placed = (P("tm", "chan"), P())
    return jax.shard_map(body, mesh=mesh, in_specs=placed, out_specs=P("chan"), check_vma=False)
```

```python
import functools

import jax
import jax.numpy as jnp
from jax import lax
from jax.experimental import pallas as pl
from jax.experimental.pallas import tpu as pltpu
from jax.sharding import PartitionSpec as P

LANES = 128
MESH = pl.DeviceIdType.MESH


def round_up(value, to):
    return (value + to - 1) // to * to


def flip(place, bits):
    out, bit = place, 1
    while bit <= bits:
        if bits & bit:
            out = out + bit * (1 - 2 * lax.rem(lax.div(place, bit), 2))
        bit *= 2
    return out


def kernel(count, chans, rows, tiles, halo, offs_ref, x_ref, out_ref, recv, *rest):
    levels = rest[:-5]
    send_sem, recv_sem, edge_sem, send_sem2, recv_sem2 = rest[-5:]
    me = lax.axis_index("tm")
    col = lax.axis_index("chan")
    total = count * rows
    body = tiles
    full = tiles + halo
    at_end = me == count - 1
    no_next = me * chans + col == count * chans - 1

    barrier = pltpu.get_barrier_semaphore()
    for j in range(1, count):
        pl.semaphore_signal(barrier, inc=1, device_id=(flip(me, j), col), device_id_type=MESH)
    if chans > 1:
        @pl.when(jnp.logical_and(at_end, col < chans - 1))
        def _():
            for t in range(count):
                pl.semaphore_signal(barrier, inc=1, device_id=(t, jnp.minimum(col + 1, chans - 1)), device_id_type=MESH)
    pl.semaphore_wait(barrier, count - 1 + jnp.where(col > 0, 1, 0))

    def to_peer(j, size):
        k = flip(me, j)
        return pltpu.make_async_remote_copy(
            src_ref=x_ref.at[pl.ds(k * body, size)],
            dst_ref=recv.at[me, pl.ds(0, size)],
            send_sem=send_sem.at[j],
            recv_sem=recv_sem.at[me],
            device_id=(k, col),
            device_id_type=MESH,
        )

    def both(j, act):
        @pl.when(flip(me, j) == count - 1)
        def _():
            act(to_peer(j, body))

        @pl.when(flip(me, j) != count - 1)
        def _():
            act(to_peer(j, full))

    def edge():
        return pltpu.make_async_remote_copy(
            src_ref=x_ref.at[pl.ds(0, halo)],
            dst_ref=recv.at[me, pl.ds(body, halo)],
            send_sem=edge_sem.at[0],
            recv_sem=recv_sem.at[me],
            device_id=(count - 1, jnp.maximum(col - 1, 0)),
            device_id_type=MESH,
        )

    def own(size):
        return pltpu.make_async_copy(
            x_ref.at[pl.ds(me * body, size)], recv.at[me, pl.ds(0, size)], recv_sem.at[me]
        )

    for j in reversed(range(1, count)):
        both(j, lambda copy: copy.start())
    if chans > 1:
        @pl.when(col > 0)
        def _():
            edge().start()

    @pl.when(at_end)
    def _():
        own(body).start()

    @pl.when(me != count - 1)
    def _():
        own(full).start()

    @pl.when(no_next)
    def _():
        for t in range(count):
            recv[t, pl.ds(body, halo)] = jnp.zeros((halo, rows, LANES), jnp.float32)

    def arrived(t):
        def wait(size):
            part = recv.at[t, pl.ds(0, size)]
            pltpu.make_async_copy(part, part, recv_sem.at[t]).wait()

        @pl.when(no_next)
        def _():
            wait(body)

        @pl.when(me * chans + col != count * chans - 1)
        def _():
            wait(full)

    def node(length, block, slot=0, inner=0):
        at = length.bit_length() - 1
        wide = tiles + (total - 2 * length + LANES - 1) // LANES
        lane = lax.broadcasted_iota(jnp.int32, (wide, LANES), 1)

        def load(which, d, start):
            if length == 1:
                return recv[slot, pl.ds(start, wide), 2 * inner + which]
            return levels[at - 1][2 * block + which, d, pl.ds(start, wide)]

        peak = None
        for half in range(length):
            low = load(0, half, 0)
            here = load(1, half, 0)
            ahead = load(1, half, 1)
            for d in (2 * half, 2 * half + 1):
                by = offs_ref[2 * length + d]
                mixed = jnp.where(lane >= by, here, ahead)
                value = low + pltpu.roll(mixed, lax.rem(LANES - by, LANES), 1)
                if 2 * length < total:
                    levels[at][block, d, pl.ds(0, wide)] = value
                else:
                    peak = value if peak is None else jnp.maximum(peak, value)
        return peak

    peak, done = None, set()
    for j in list(range(count // 2)) + list(reversed(range(count // 2, count))):
        slot = flip(me, j)
        arrived(slot)
        done.add(j)
        length = 1
        while length < rows:
            for inner in range(rows // (2 * length)):
                peak = node(length, slot * (rows // (2 * length)) + inner, slot, inner)
            length *= 2
        step = 1
        while step < count and done.issuperset(range(j // (2 * step) * 2 * step, (j // (2 * step) + 1) * 2 * step)):
            peak = node(step * rows, flip(lax.div(me, 2 * step), j // (2 * step)))
            step *= 2

    mine = pl.ds(me * tiles, tiles)
    out_ref[mine] = peak
    for j in range(1, count):
        both(j, lambda copy: copy.wait_send())
    if chans > 1:
        @pl.when(col > 0)
        def _():
            edge().wait_send()

    def result(j, t):
        part = out_ref.at[pl.ds(t * tiles, tiles)]
        return pltpu.make_async_remote_copy(
            src_ref=part,
            dst_ref=part,
            send_sem=send_sem2.at[j],
            recv_sem=recv_sem2.at[t],
            device_id=(flip(me, j), col),
            device_id_type=MESH,
        )

    for j in reversed(range(1, count)):
        result(j, me).start()
    for j in range(1, count):
        result(j, flip(me, j)).wait_recv()
    for j in range(1, count):
        result(j, me).wait_send()


def local(count, chans, spectrum, offsets):
    rows, span = spectrum.shape
    total = count * rows
    tiles = span // LANES // count
    halo = (total - 1 + LANES - 1) // LANES
    x = spectrum.reshape(rows, span // LANES, LANES).transpose(1, 0, 2)
    deep = round_up(tiles + halo, 8) + 8
    scratch = [pltpu.VMEM((count, deep, rows, LANES), jnp.float32)]
    length = 2
    while length < total:
        scratch.append(pltpu.VMEM((total // length, length, deep, LANES), jnp.float32))
        length *= 2
    dma = pltpu.SemaphoreType.DMA
    scratch += [dma((count,)), dma((count,)), dma((1,)), dma((count,)), dma((count,))]
    peak = pl.pallas_call(
        functools.partial(kernel, count, chans, rows, tiles, halo),
        out_shape=jax.ShapeDtypeStruct((count * tiles, LANES), jnp.float32),
        in_specs=[pl.BlockSpec(memory_space=pltpu.SMEM), pl.BlockSpec(memory_space=pl.ANY)],
        out_specs=pl.BlockSpec(memory_space=pltpu.VMEM),
        scratch_shapes=scratch,
        compiler_params=pltpu.CompilerParams(collective_id=0, has_side_effects=True),
    )(offsets, x)
    return peak.reshape(span)


def solution(mesh):
    body = functools.partial(local, mesh.shape["tm"], mesh.shape["chan"])
    placed = (P("tm", "chan"), P())
    return jax.shard_map(body, mesh=mesh, in_specs=placed, out_specs=P("chan"), check_vma=False)
```

```python
import functools

import jax
import jax.numpy as jnp
from jax import lax
from jax.experimental import pallas as pl
from jax.experimental.pallas import tpu as pltpu
from jax.sharding import PartitionSpec as P

LANES = 128
MESH = pl.DeviceIdType.MESH


def round_up(value, to):
    return (value + to - 1) // to * to


def flip(place, bits):
    out, bit = place, 1
    while bit <= bits:
        if bits & bit:
            out = out + bit * (1 - 2 * lax.rem(lax.div(place, bit), 2))
        bit *= 2
    return out


def kernel(count, chans, rows, tiles, halo, offs_ref, x_ref, out_ref, recv, *rest):
    levels = rest[:-5]
    send_sem, recv_sem, edge_sem, send_sem2, recv_sem2 = rest[-5:]
    me = lax.axis_index("tm")
    col = lax.axis_index("chan")
    total = count * rows
    body = tiles
    full = tiles + halo
    at_end = me == count - 1
    no_next = me * chans + col == count * chans - 1

    barrier = pltpu.get_barrier_semaphore()
    for j in range(1, count):
        pl.semaphore_signal(barrier, inc=1, device_id=(flip(me, j), col), device_id_type=MESH)
    if chans > 1:
        @pl.when(jnp.logical_and(at_end, col < chans - 1))
        def _():
            for t in range(count):
                pl.semaphore_signal(barrier, inc=1, device_id=(t, jnp.minimum(col + 1, chans - 1)), device_id_type=MESH)
    pl.semaphore_wait(barrier, count - 1 + jnp.where(col > 0, 1, 0))

    def to_peer(j, size):
        k = flip(me, j)
        return pltpu.make_async_remote_copy(
            src_ref=x_ref.at[pl.ds(k * body, size)],
            dst_ref=recv.at[me, pl.ds(0, size)],
            send_sem=send_sem.at[j],
            recv_sem=recv_sem.at[me],
            device_id=(k, col),
            device_id_type=MESH,
        )

    def both(j, act):
        @pl.when(flip(me, j) == count - 1)
        def _():
            act(to_peer(j, body))

        @pl.when(flip(me, j) != count - 1)
        def _():
            act(to_peer(j, full))

    def edge():
        return pltpu.make_async_remote_copy(
            src_ref=x_ref.at[pl.ds(0, halo)],
            dst_ref=recv.at[me, pl.ds(body, halo)],
            send_sem=edge_sem.at[0],
            recv_sem=recv_sem.at[me],
            device_id=(count - 1, jnp.maximum(col - 1, 0)),
            device_id_type=MESH,
        )

    def own(size):
        return pltpu.make_async_copy(
            x_ref.at[pl.ds(me * body, size)], recv.at[me, pl.ds(0, size)], recv_sem.at[me]
        )

    if chans > 1:
        @pl.when(col > 0)
        def _():
            edge().start()

    for j in reversed(range(1, count)):
        both(j, lambda copy: copy.start())

    @pl.when(at_end)
    def _():
        own(body).start()

    @pl.when(me != count - 1)
    def _():
        own(full).start()

    @pl.when(no_next)
    def _():
        for t in range(count):
            recv[t, pl.ds(body, halo)] = jnp.zeros((halo, rows, LANES), jnp.float32)

    def arrived(t):
        def wait(size):
            part = recv.at[t, pl.ds(0, size)]
            pltpu.make_async_copy(part, part, recv_sem.at[t]).wait()

        @pl.when(no_next)
        def _():
            wait(body)

        @pl.when(me * chans + col != count * chans - 1)
        def _():
            wait(full)

    def node(length, block, slot=0, inner=0):
        at = length.bit_length() - 1
        wide = tiles + (total - 2 * length + LANES - 1) // LANES
        lane = lax.broadcasted_iota(jnp.int32, (wide, LANES), 1)

        def load(which, d, start):
            if length == 1:
                return recv[slot, pl.ds(start, wide), 2 * inner + which]
            return levels[at - 1][2 * block + which, d, pl.ds(start, wide)]

        peak = None
        for half in range(length):
            low = load(0, half, 0)
            here = load(1, half, 0)
            ahead = load(1, half, 1)
            for d in (2 * half, 2 * half + 1):
                by = offs_ref[2 * length + d]
                mixed = jnp.where(lane >= by, here, ahead)
                value = low + pltpu.roll(mixed, lax.rem(LANES - by, LANES), 1)
                if 2 * length < total:
                    levels[at][block, d, pl.ds(0, wide)] = value
                else:
                    peak = value if peak is None else jnp.maximum(peak, value)
        return peak

    peak, done = None, set()
    for j in list(range(count // 2)) + list(reversed(range(count // 2, count))):
        slot = flip(me, j)
        arrived(slot)
        done.add(j)
        length = 1
        while length < rows:
            for inner in range(rows // (2 * length)):
                peak = node(length, slot * (rows // (2 * length)) + inner, slot, inner)
            length *= 2
        step = 1
        while step < count and done.issuperset(range(j // (2 * step) * 2 * step, (j // (2 * step) + 1) * 2 * step)):
            peak = node(step * rows, flip(lax.div(me, 2 * step), j // (2 * step)))
            step *= 2

    mine = pl.ds(me * tiles, tiles)
    out_ref[mine] = peak
    for j in range(1, count):
        both(j, lambda copy: copy.wait_send())
    if chans > 1:
        @pl.when(col > 0)
        def _():
            edge().wait_send()

    def result(j, t):
        part = out_ref.at[pl.ds(t * tiles, tiles)]
        return pltpu.make_async_remote_copy(
            src_ref=part,
            dst_ref=part,
            send_sem=send_sem2.at[j],
            recv_sem=recv_sem2.at[t],
            device_id=(flip(me, j), col),
            device_id_type=MESH,
        )

    for j in reversed(range(1, count)):
        result(j, me).start()
    for j in range(1, count):
        result(j, flip(me, j)).wait_recv()
    for j in range(1, count):
        result(j, me).wait_send()


def local(count, chans, spectrum, offsets):
    rows, span = spectrum.shape
    total = count * rows
    tiles = span // LANES // count
    halo = (total - 1 + LANES - 1) // LANES
    x = spectrum.reshape(rows, span // LANES, LANES).transpose(1, 0, 2)
    deep = round_up(tiles + halo, 8) + 8
    scratch = [pltpu.VMEM((count, deep, rows, LANES), jnp.float32)]
    length = 2
    while length < total:
        scratch.append(pltpu.VMEM((total // length, length, deep, LANES), jnp.float32))
        length *= 2
    dma = pltpu.SemaphoreType.DMA
    scratch += [dma((count,)), dma((count,)), dma((1,)), dma((count,)), dma((count,))]
    peak = pl.pallas_call(
        functools.partial(kernel, count, chans, rows, tiles, halo),
        out_shape=jax.ShapeDtypeStruct((count * tiles, LANES), jnp.float32),
        in_specs=[pl.BlockSpec(memory_space=pltpu.SMEM), pl.BlockSpec(memory_space=pl.ANY)],
        out_specs=pl.BlockSpec(memory_space=pltpu.VMEM),
        scratch_shapes=scratch,
        compiler_params=pltpu.CompilerParams(collective_id=0, has_side_effects=True),
    )(offsets, x)
    return peak.reshape(span)


def solution(mesh):
    body = functools.partial(local, mesh.shape["tm"], mesh.shape["chan"])
    placed = (P("tm", "chan"), P())
    return jax.shard_map(body, mesh=mesh, in_specs=placed, out_specs=P("chan"), check_vma=False)
```
